32 devices in a mesh: front: 2 (over y), row: 4 (over z), col: 4 (over x, core).
Axes of the slice: x: 2, y: 2, z: 4, core: 2. Of those that a mesh axis runs over, the one named last changes fastest.
Arguments:
- pivot: float32 [2, 512, 512], P('front', ('row', 'col')), may hold values from -1 to 8
- col_ut: bfloat16 [2, 4, 96, 512], P('front', 'row', None, 'col'), may hold values from -6 to 6
- col_vt: bfloat16 [2, 4, 96, 512], P('front', 'row', None, 'col'), may hold values from -0.25 to 0.25
- col_rank: int32 [2, 4], P('front', 'row'), may hold values from 32 to 96
- row_ut: bfloat16 [2, 4, 96, 512], P('front', 'col', None, 'row'), may hold values from -6 to 6
- row_vt: bfloat16 [2, 4, 96, 512], P('front', 'col', None, 'row'), may hold values from -0.625 to 0.625
- row_rank: int32 [2, 4], P('front', 'col'), may hold values from 32 to 96
- cb_ut: bfloat16 [2, 4, 4, 96, 512], P('front', 'row', 'col'), may hold values from -6 to 6
- cb_vt: bfloat16 [2, 4, 4, 96, 512], P('front', 'row', 'col'), may hold values from -0.625 to 0.625
- cb_rank: int32 [2, 4, 4], P('front', 'row', 'col'), may hold values from 32 to 96
- parent_map: int32 [2, 4], P('front'), may hold values from 0 to 7, as said below
Outputs:
- parent_tiles: bfloat16 [2, 8, 4, 512, 512], P('front', 'row', 'col')
The draws below stay inside these ranges and needn't reach their ends.
Inputs may be any that keep to these rules, and one draw needn't show every extreme that they name: `parent_map`: for every front the entries are distinct; entry 0 is 4, and 0 and 7 both appear.
All inputs are finite; a program needn't handle non-finite values.
Results may differ from the reference program's by a relative error of at most 0.0062.
Values may be sent and summed in bfloat16 or wider, within the bound.
A program may use at most 64 MiB of HBM per device.

```python
import math
import jax
import jax.numpy as jnp
from jax import lax

TILE = 512
RANK = 96
NS_ITERS = 2
TD = 1
NC = 4
NP = 8
FRONTS = 2
PARENTS = 1
N_COL = 4


def draw_pivot(key, part):
    key_off, key_diag = jax.random.split(key, 2)
    spread = 1.2 * TILE ** (-0.5)
    offdiag = jax.random.normal(key_off, (FRONTS, TILE, TILE), jnp.float32) * spread
    levels = jax.random.uniform(key_diag, (FRONTS, TILE), jnp.float32, math.log(4.0), math.log(8.0))
    diagonal = jnp.exp(levels)
    eye = jnp.eye(TILE, dtype=jnp.float32)
    return offdiag * (1.0 - eye)[None] + diagonal[:, :, None] * eye[None]


def pick_targets(single):
    key_pick, key_order = jax.random.split(single, 2)
    values = jnp.arange(NP, dtype=jnp.int32)
    scores = jax.random.permutation(key_pick, NP).astype(jnp.int32)
    at_ends = ((values == 0) | (values == NP - 1)).astype(jnp.int32)
    reserved = (values == NC).astype(jnp.int32)
    scores = scores + 2 * NP * at_ends - 4 * NP * reserved
    ranking = jnp.argsort(-scores, stable=True).astype(jnp.int32)
    chosen = jax.random.permutation(key_order, ranking[:NC - 1]).astype(jnp.int32)
    return jnp.concatenate([jnp.full((1,), NC, jnp.int32), chosen]).astype(jnp.int32)


def draw_parent_map(key, part):
    front_keys = jax.random.split(jax.random.fold_in(key, 7), FRONTS)
    return jax.vmap(pick_targets)(front_keys).astype(jnp.int32)


def set_ends(entries, stream_key, smallest, high):
    shape = entries.shape
    place = [jax.random.randint(jax.random.fold_in(stream_key, axis), (), 0, shape[axis]) for axis in range(len(shape))]
    entries = entries.at[tuple(place)].set(smallest)
    longest = shape.index(max(shape))
    place[longest] = (place[longest] + 1) % shape[longest]
    return entries.at[tuple(place)].set(high)


def level_of(key, dims, shards, least, largest):
    loudness, own = 1.0, jax.random.fold_in(key, 6)
    for axis_at, blocks in shards:
        heights = jnp.exp(jax.random.uniform(jax.random.fold_in(own, axis_at), (blocks,), jnp.float32, least / len(shards), largest / len(shards)))
        loudness = loudness * jnp.repeat(heights, dims[axis_at] // blocks).reshape([-1 if axis == axis_at else 1 for axis in range(len(dims))])
    return loudness


def centred(key, shape, scale, reach, shards=(), held_as=jnp.bfloat16):
    drawn = jax.random.normal(key, shape, jnp.float32) * scale
    if len(shards) > 0:
        drawn = level_of(key, shape, shards, -0.22, 0.18) * drawn
    return jnp.clip(drawn, min=-reach, max=reach).astype(held_as)


def setup_inputs(seed: int = 0) -> dict:
    streams_of = jax.random.split(jax.random.key(seed), 12)
    pivot = draw_pivot(jax.random.fold_in(streams_of[11], 71), 0)
    col_ut = centred(streams_of[1], (FRONTS, NC, RANK, TILE), 1.0, 6.0, ((0, 2), (1, 4), (3, 4)))
    col_vt = centred(streams_of[2], (FRONTS, NC, RANK, TILE), TILE ** -0.5, 0.25, ((0, 2), (1, 4), (3, 4)))
    col_rank = set_ends(jax.random.randint(streams_of[3], (FRONTS, NC), RANK // 3, RANK + 1), jax.random.fold_in(streams_of[3], 1), RANK // 3, RANK).astype(jnp.int32)
    row_ut = centred(streams_of[4], (FRONTS, NC, RANK, TILE), 1.0, 6.0, ((0, 2), (1, 4), (3, 4)))
    row_vt = centred(streams_of[5], (FRONTS, NC, RANK, TILE), RANK ** -0.5, 0.625, ((0, 2), (1, 4), (3, 4)))
    row_rank = set_ends(jax.random.randint(streams_of[6], (FRONTS, NC), RANK // 3, RANK + 1), jax.random.fold_in(streams_of[6], 1), RANK // 3, RANK).astype(jnp.int32)
    cb_ut = centred(streams_of[7], (FRONTS, NC, NC, RANK, TILE), 1.0, 6.0, ((0, 2), (1, 4), (2, 4)))
    cb_vt = centred(streams_of[8], (FRONTS, NC, NC, RANK, TILE), RANK ** -0.5, 0.625, ((0, 2), (1, 4), (2, 4)))
    cb_rank = set_ends(jax.random.randint(streams_of[9], (FRONTS, NC, NC), RANK // 3, RANK + 1), jax.random.fold_in(streams_of[9], 1), RANK // 3, RANK).astype(jnp.int32)
    parent_map = draw_parent_map(jax.random.fold_in(streams_of[11], 71), 0)
    return {"pivot": pivot, "col_ut": col_ut, "col_vt": col_vt, "col_rank": col_rank, "row_ut": row_ut, "row_vt": row_vt, "row_rank": row_rank, "cb_ut": cb_ut, "cb_vt": cb_vt, "cb_rank": cb_rank, "parent_map": parent_map}


HIGH = lax.Precision.HIGHEST


def invert(matrix):
    eye = jnp.eye(matrix.shape[0], dtype=jnp.float32)
    approx = eye / jnp.diagonal(matrix)[None, :]
    for step in range(NS_ITERS):
        approx = jnp.dot(approx, 2.0 * eye - jnp.dot(matrix, approx, precision=HIGH), precision=HIGH)
    return approx


def ranked(factor, rank):
    levels = jnp.arange(factor.shape[-2], dtype=jnp.int32)[:, None]
    keep = levels < rank[..., None, None]
    return jnp.where(keep, factor, jnp.zeros_like(factor)).astype(jnp.bfloat16)


def child(pivot, col_ut, col_vt, col_rank, row_ut, row_vt, row_rank, cb_ut, cb_vt, cb_rank, parent_map):
    inverse = invert(pivot)
    left_col = ranked(col_ut, col_rank)
    right_col = ranked(col_vt, col_rank)
    lower = jnp.einsum('atx,xy->aty', right_col.astype(jnp.float32), inverse, precision=HIGH).astype(jnp.bfloat16)
    upper_left = ranked(row_ut, row_rank)
    upper_right = ranked(row_vt, row_rank)
    core = jnp.einsum('iax,jbx->ijab', lower.astype(jnp.float32), upper_left.astype(jnp.float32)).astype(jnp.bfloat16)
    update = jnp.einsum('ijab,iax->ijbx', core.astype(jnp.float32), left_col.astype(jnp.float32)).astype(jnp.bfloat16)
    block_left = ranked(cb_ut, cb_rank)
    block_right = ranked(cb_vt, cb_rank)

    def one_row(pieces):
        left_part, right_part, update_part = pieces
        left = jnp.concatenate([left_part, -update_part], axis=1).astype(jnp.float32)
        right = jnp.concatenate([right_part, upper_right], axis=1).astype(jnp.float32)
        return jnp.einsum('jkx,jky->jxy', left, right).astype(jnp.bfloat16)

    schur = lax.map(one_row, (block_left, block_right, update))
    count = parent_map.shape[0]
    places = jnp.arange(count, dtype=jnp.int32)
    targets = jnp.arange(NP, dtype=jnp.int32)
    onehot = (parent_map[None, :] == targets[:, None]).astype(jnp.int32)
    source = jnp.sum(onehot * places[None, :], axis=1).astype(jnp.int32)
    present = jnp.sum(onehot, axis=1) > 0
    placed = schur[source][:, source]
    keep = present[:, None] & present[None, :]
    return jnp.where(keep[:, :, None, None], placed, jnp.zeros_like(placed))


def reference(pivot, col_ut, col_vt, col_rank, row_ut, row_vt, row_rank, cb_ut, cb_vt, cb_rank, parent_map):
    arrays = (pivot, col_ut, col_vt, col_rank, row_ut, row_vt, row_rank, cb_ut, cb_vt, cb_rank, parent_map)
    paired = tuple(item.reshape((PARENTS, 2) + item.shape[1:]) for item in arrays)

    def one_parent(group):
        first = child(*[item[0] for item in group])
        second = child(*[item[1] for item in group])
        return (first.astype(jnp.float32) + second.astype(jnp.float32)).astype(jnp.bfloat16)

    parents = lax.map(one_parent, paired)
    laid = parents.reshape(PARENTS, NP, N_COL, 2, TD, TILE, TILE)
    laid = jnp.transpose(laid, (0, 3, 1, 2, 4, 5, 6))
    return laid.reshape(PARENTS * 2, NP, N_COL * TD, TILE, TILE)
```

```python
import functools

import jax
import jax.numpy as jnp
from jax import lax
from jax.experimental import pallas as pl
from jax.experimental.pallas import tpu as pltpu
from jax.sharding import PartitionSpec as P

MESH = pl.DeviceIdType.MESH
F32 = jnp.float32
BF16 = jnp.bfloat16


def mm(a, b, dims):
    return lax.dot_general(a, b, (dims, ((), ())), preferred_element_type=F32)


def kernel(
    n_row,
    n_col,
    pivot,
    col_ut,
    col_vt,
    row_ut,
    row_vt,
    cb_ut,
    cb_vt,
    col_rank,
    row_rank,
    cb_rank,
    pmap,
    out,
    mbuf,
    fbuf,
    ubuf,
    vbuf,
    su,
    sv,
    yu,
    yv,
    yd,
    yr,
    zu,
    zv,
    zd,
    zr,
    rsem_p,
    ssem_p,
    rsem_c,
    ssem_c,
    rsem_s,
    ssem_s,
    rsem_y,
    ssem_y,
):
    front, r, c = lax.axis_index("front"), lax.axis_index("row"), lax.axis_index("col")
    n_x = n_col // 2
    x, core = c // 2, c % 2
    partner = 2 * x + 1 - core
    sibling = front + 1 - 2 * (front % 2)
    half = front % 2
    peers = [lax.rem(x + k, n_x) * 2 + core for k in range(1, n_x)]
    wc, wr = col_ut.shape[-1], row_ut.shape[-1]
    rank_dim, tile = cb_ut.shape[-2], cb_ut.shape[-1]
    mr = pivot.shape[1]
    has_left, has_right = r > 0, r < n_row - 1

    barrier = pltpu.get_barrier_semaphore()

    def greet(target):
        pl.semaphore_signal(barrier, inc=1, device_id=target, device_id_type=MESH)

    greet((sibling, r, c))
    greet((front, r, partner))
    for p in peers:
        greet((front, r, p))

    @pl.when(has_left)
    def _():
        greet((front, r - 1, c))

    @pl.when(has_right)
    def _():
        greet((front, r + 1, c))

    me = r * n_col + c
    rows_at = lax.broadcasted_iota(jnp.int32, (mr, tile), 0) + me * mr
    lanes_at = lax.broadcasted_iota(jnp.int32, (mr, tile), 1)
    on_diag = rows_at == lanes_at
    mine = pivot[0]
    inv = 1.0 / jnp.sum(jnp.where(on_diag, mine, 0.0), axis=1, keepdims=True)
    mbuf[me] = jnp.where(on_diag, inv, mine * inv).astype(BF16)

    def masked(value, rank):
        level = lax.broadcasted_iota(jnp.int32, value.shape, 0)
        return jnp.where(level < rank, value.astype(F32), 0.0).astype(BF16)

    fbuf[me] = jnp.concatenate(
        [
            col_ut[0, 0],
            masked(col_vt[0, 0], col_rank[0, 0]),
            masked(row_ut[0, 0], row_rank[0, 0]),
            row_vt[0, 0],
        ],
        axis=1,
    )
    ubuf[r] = masked(cb_ut[0, 0, 0], cb_rank[0, 0, 0])
    vbuf[r] = cb_vt[0, 0, 0]

    greeted = 2 + len(peers) + has_left.astype(jnp.int32) + has_right.astype(jnp.int32)
    pl.semaphore_wait(barrier, greeted)

    def copy(ref, send, recv, target):
        return pltpu.make_async_remote_copy(
            src_ref=ref, dst_ref=ref, send_sem=send, recv_sem=recv, device_id=target, device_id_type=MESH
        )

    left_dev, right_dev = (front, r - 1, c), (front, r + 1, c)
    partner_dev = (front, r, partner)
    panel = (mbuf, fbuf)

    def pcopy(t, q, cc, k, target):
        slot = q * n_col + cc
        return copy(panel[t].at[slot], ssem_p.at[t, slot, k], rsem_p.at[t, slot], target)

    def ccopy(t, q, k, target):
        return copy((ubuf, vbuf)[t].at[q], ssem_c.at[t, q, k], rsem_c.at[t, q], target)

    def z_start(make, q, came_right, came_left):
        if came_right:

            @pl.when(has_right)
            def _():
                make(2, right_dev).start()

        if came_left:

            @pl.when(has_left)
            def _():
                make(1, left_dev).start()

    def x_start(t, q):
        for k, p in enumerate(peers):
            pcopy(t, q, c, 3 + k, (front, r, p)).start()
        pcopy(t, q, c, 0, partner_dev).start()

    def hop(s):
        if s == 0:
            for t in range(2):
                z_start(lambda k, d, t=t: pcopy(t, r, c, k, d), r, True, True)
                x_start(t, r)
            for t in range(2):
                z_start(lambda k, d, t=t: ccopy(t, r, k, d), r, True, True)
            return

        def arrive(q, right):
            for t in range(2):
                pcopy(t, q, c, 0, partner_dev).wait_recv()
                z_start(lambda k, d, t=t: pcopy(t, q, c, k, d), q, right, not right)
                x_start(t, q)
            for t in range(2):
                ccopy(t, q, 0, partner_dev).wait_recv()
                z_start(lambda k, d, t=t: ccopy(t, q, k, d), q, right, not right)

        @pl.when(r - s >= 0)
        def _():
            arrive(r - s, True)

        @pl.when(r + s < n_row)
        def _():
            arrive(r + s, False)

    for s in range(n_row):
        hop(s)

    def find(wanted):
        at, found = jnp.int32(0), jnp.int32(0)
        for i in range(pmap.shape[1]):
            hit = pmap[0, i] == wanted
            at, found = jnp.where(hit, i, at), jnp.where(hit, 1, found)
        return at, found.astype(F32)

    i_at = [find(2 * r + u) for u in range(2)]
    j_own, j_sib = find(2 * c + half), find(2 * c + 1 - half)

    def kept(value, flag):
        return (value.astype(F32) * flag).astype(BF16)

    for u in range(2):
        at, found = i_at[u]
        su[c, u] = kept(ubuf[at], found)
        sv[c, u] = vbuf[at]

    stacks = (su, sv)

    def scopy(t, cc, k, target):
        return copy(stacks[t].at[cc], ssem_s.at[t, cc, k], rsem_s.at[t, cc], target)

    for t in range(2):
        for k, p in enumerate(peers):
            scopy(t, c, 1 + k, (front, r, p)).start()
        scopy(t, c, 0, partner_dev).start()

    for s in range(n_row):

        def relay(q):
            for t in range(2):
                for p in peers:
                    pcopy(t, q, p, 0, partner_dev).wait_recv()
                    pcopy(t, q, p, 0, partner_dev).start()

        @pl.when(r - s >= 0)
        def _():
            relay(r - s)

        if s > 0:

            @pl.when(r + s < n_row)
            def _():
                relay(r + s)

    others = [lax.rem(x + k, n_x) * 2 + 1 - core for k in range(n_x)]
    for q in range(n_row):
        for t in range(2):
            for p in others:
                pcopy(t, q, p, 0, partner_dev).wait_recv()

    pivots = mbuf[...].reshape(tile, tile)
    diag_blocks = []
    lane_block = 128
    for b in range(tile // lane_block):
        total = jnp.zeros((1, lane_block), F32)
        for d in range(lane_block // mr):
            dev = b * (lane_block // mr) + d
            piece = mbuf[dev, :, b * lane_block : (b + 1) * lane_block].astype(F32)
            at_r = lax.broadcasted_iota(jnp.int32, piece.shape, 0) + d * mr
            at_l = lax.broadcasted_iota(jnp.int32, piece.shape, 1)
            total = total + jnp.sum(jnp.where(at_r == at_l, piece, 0.0), axis=0, keepdims=True)
        diag_blocks.append(total)
    diag = jnp.concatenate(diag_blocks, axis=1)

    def col_piece(at, first):
        return jnp.concatenate(
            [fbuf[at * n_col + k][:, first : first + wc] for k in range(n_col)], axis=1
        )

    def row_piece(at, first):
        return jnp.concatenate(
            [fbuf[k * n_col + at][:, first : first + wr] for k in range(n_row)], axis=1
        )

    v = jnp.concatenate([col_piece(i_at[u][0], wc) for u in range(2)], axis=0)
    v32 = v.astype(F32)
    t = v
    for step in range(3):
        t32 = v32 - (mm(t, pivots, ((1,), (0,))) - t.astype(F32) * diag)
        t = t32.astype(BF16)
    lower = (t32 * diag).astype(BF16)
    col_u = [col_piece(i_at[u][0], 0) for u in range(2)]

    def updates(j):
        at, found = j
        core_ = mm(lower, row_piece(at, 2 * wc), ((1,), (1,))).astype(BF16)
        return [
            (
                mm(core_[u * rank_dim : (u + 1) * rank_dim], col_u[u], ((0,), (0,)))
                * (-found * i_at[u][1])
            ).astype(BF16)
            for u in range(2)
        ]

    ends = ((yd, zd), (yr, zr), (yu, zu), (yv, zv))

    def ycopy(t):
        return pltpu.make_async_remote_copy(
            src_ref=ends[t][0],
            dst_ref=ends[t][1],
            send_sem=ssem_y.at[t],
            recv_sem=rsem_y.at[t],
            device_id=(sibling, r, c),
            device_id_type=MESH,
        )

    yr[...] = row_piece(j_sib[0], 2 * wc + wr)
    ycopy(1).start()
    for u, value in enumerate(updates(j_sib)):
        yd[u] = value
    ycopy(0).start()

    for t in range(2):
        for p in peers:
            scopy(t, p, 0, partner_dev).wait_recv()
            scopy(t, p, 0, partner_dev).start()
    for t in range(2):
        for p in others:
            scopy(t, p, 0, partner_dev).wait_recv()
    for u in range(2):
        yu[u] = kept(su[j_sib[0], u], j_sib[1])
    ycopy(2).start()
    for u in range(2):
        yv[u] = sv[j_sib[0], u]
    ycopy(3).start()

    own = updates(j_own)
    own_r = row_piece(j_own[0], 2 * wc + wr)
    lefts = [
        jnp.concatenate([kept(su[j_own[0], u], j_own[1]), own[u]], axis=0) for u in range(2)
    ]
    rights = [jnp.concatenate([sv[j_own[0], u], own_r], axis=0) for u in range(2)]
    for t in range(4):
        ycopy(t).wait_recv()
    for u in range(2):
        left = jnp.concatenate([lefts[u], zu[u], zd[u]], axis=0)
        right = jnp.concatenate([rights[u], zv[u], zr[...]], axis=0)
        out[0, u, 0] = mm(left, right, ((0,), (0,))).astype(BF16)

    for t in range(4):
        ycopy(t).wait_send()
    for t in range(2):
        for k, p in enumerate(peers):
            scopy(t, c, 1 + k, partner_dev).wait_send()
            scopy(t, p, 0, partner_dev).wait_send()
        scopy(t, c, 0, partner_dev).wait_send()
        for q in range(n_row):
            for k, p in enumerate(peers):
                pcopy(t, q, c, 3 + k, partner_dev).wait_send()
                pcopy(t, q, p, 0, partner_dev).wait_send()
            pcopy(t, q, c, 0, partner_dev).wait_send()

            @pl.when((q <= r) & has_right)
            def _():
                pcopy(t, q, c, 2, partner_dev).wait_send()
                ccopy(t, q, 2, partner_dev).wait_send()

            @pl.when((q >= r) & has_left)
            def _():
                pcopy(t, q, c, 1, partner_dev).wait_send()
                ccopy(t, q, 1, partner_dev).wait_send()


def shards(
    n_row,
    n_col,
    pivot,
    col_ut,
    col_vt,
    col_rank,
    row_ut,
    row_vt,
    row_rank,
    cb_ut,
    cb_vt,
    cb_rank,
    parent_map,
):
    n_x = n_col // 2
    mr = pivot.shape[1]
    rank_dim, tile = cb_ut.shape[-2], cb_ut.shape[-1]
    width = 2 * col_ut.shape[-1] + 2 * row_ut.shape[-1]
    vmem = pl.BlockSpec(memory_space=pltpu.VMEM)
    smem = pl.BlockSpec(memory_space=pltpu.SMEM)
    pair = (2, rank_dim, tile)
    dma = pltpu.SemaphoreType.DMA
    return pl.pallas_call(
        functools.partial(kernel, n_row, n_col),
        out_shape=jax.ShapeDtypeStruct((1, 2, 1, tile, tile), BF16),
        in_specs=[vmem] * 7 + [smem] * 4,
        out_specs=vmem,
        scratch_shapes=[
            pltpu.VMEM((n_row * n_col, mr, tile), BF16),
            pltpu.VMEM((n_row * n_col, rank_dim, width), BF16),
            pltpu.VMEM((n_row, rank_dim, tile), BF16),
            pltpu.VMEM((n_row, rank_dim, tile), BF16),
            pltpu.VMEM((n_col,) + pair, BF16),
            pltpu.VMEM((n_col,) + pair, BF16),
            pltpu.VMEM(pair, BF16),
            pltpu.VMEM(pair, BF16),
            pltpu.VMEM(pair, BF16),
            pltpu.VMEM(pair[1:], BF16),
            pltpu.VMEM(pair, BF16),
            pltpu.VMEM(pair, BF16),
            pltpu.VMEM(pair, BF16),
            pltpu.VMEM(pair[1:], BF16),
            dma((2, n_row * n_col)),
            dma((2, n_row * n_col, 2 + n_x)),
            dma((2, n_row)),
            dma((2, n_row, 3)),
            dma((2, n_col)),
            dma((2, n_col, n_x)),
            dma((4,)),
            dma((4,)),
        ],
        compiler_params=pltpu.CompilerParams(
            collective_id=0, has_side_effects=True, vmem_limit_bytes=40 * 1024 * 1024
        ),
    )(
        pivot,
        col_ut,
        col_vt,
        row_ut,
        row_vt,
        cb_ut,
        cb_vt,
        col_rank,
        row_rank,
        cb_rank,
        parent_map,
    )


def solution(mesh):
    placed = (
        P("front", ("row", "col"), None),
        P("front", "row", None, "col"),
        P("front", "row", None, "col"),
        P("front", "row"),
        P("front", "col", None, "row"),
        P("front", "col", None, "row"),
        P("front", "col"),
        P("front", "row", "col", None, None),
        P("front", "row", "col", None, None),
        P("front", "row", "col"),
        P("front", None),
    )
    return jax.shard_map(
        functools.partial(shards, mesh.shape["row"], mesh.shape["col"]),
        mesh=mesh,
        in_specs=placed,
        out_specs=P("front", "row", "col", None, None),
        check_vma=False,
    )
```

```python
import functools

import jax
import jax.numpy as jnp
from jax import lax
from jax.experimental import pallas as pl
from jax.experimental.pallas import tpu as pltpu
from jax.sharding import PartitionSpec as P

MESH = pl.DeviceIdType.MESH
F32 = jnp.float32
BF16 = jnp.bfloat16


def mm(a, b, dims):
    return lax.dot_general(a, b, (dims, ((), ())), preferred_element_type=F32)


def kernel(
    n_row,
    n_col,
    pivot_hbm,
    col_ut_hbm,
    col_vt_hbm,
    row_ut_hbm,
    row_vt_hbm,
    cb_ut_hbm,
    cb_vt_hbm,
    col_rank_hbm,
    row_rank_hbm,
    cb_rank_hbm,
    pmap_hbm,
    out,
    pivot,
    col_ut,
    col_vt,
    row_ut,
    row_vt,
    col_rank,
    row_rank,
    cb_rank,
    pmap,
    mbuf,
    fbuf,
    c0,
    c1,
    c2,
    c3,
    s0,
    s1,
    s2,
    s3,
    ybuf,
    yd,
    yr,
    zbuf,
    zd,
    zr,
    in_sem,
    rsem_p,
    ssem_p,
    rsem_c,
    ssem_c,
    rsem_s,
    ssem_s,
    rsem_y,
    ssem_y,
):
    cbuf, sbuf = (c0, c1, c2, c3), (s0, s1, s2, s3)
    front, r, c = lax.axis_index("front"), lax.axis_index("row"), lax.axis_index("col")
    n_x = n_col // 2
    x, core = c // 2, c % 2
    partner = 2 * x + 1 - core
    sibling = front + 1 - 2 * (front % 2)
    half = front % 2
    peers = [lax.rem(x + k, n_x) * 2 + core for k in range(1, n_x)]
    wc, wr = col_ut.shape[-1], row_ut.shape[-1]
    rank_dim, tile = cb_ut_hbm.shape[-2], cb_ut_hbm.shape[-1]
    wide = tile // 2
    mr = pivot.shape[1]
    has_left, has_right = r > 0, r < n_row - 1

    def chunk_src(k):
        return (cb_ut_hbm, cb_vt_hbm)[k // 2].at[0, 0, 0, :, pl.ds(k % 2 * wide, wide)]

    loads = [
        pltpu.make_async_copy(src, dst, in_sem.at[k])
        for k, (src, dst) in enumerate(
            [
                (pivot_hbm, pivot),
                (col_rank_hbm, col_rank),
                (row_rank_hbm, row_rank),
                (cb_rank_hbm, cb_rank),
                (pmap_hbm, pmap),
                (col_ut_hbm, col_ut),
                (col_vt_hbm, col_vt),
                (row_ut_hbm, row_ut),
                (row_vt_hbm, row_vt),
            ]
            + [(chunk_src(k), cbuf[k].at[r]) for k in range(4)]
        )
    ]
    for load in loads:
        load.start()

    barrier = pltpu.get_barrier_semaphore()

    def greet(target):
        pl.semaphore_signal(barrier, inc=1, device_id=target, device_id_type=MESH)

    greet((sibling, r, c))
    greet((front, r, partner))
    for p in peers:
        greet((front, r, p))

    @pl.when(has_left)
    def _():
        greet((front, r - 1, c))

    @pl.when(has_right)
    def _():
        greet((front, r + 1, c))

    for load in loads:
        load.wait()
    me = r * n_col + c
    rows_at = lax.broadcasted_iota(jnp.int32, (mr, tile), 0) + me * mr
    lanes_at = lax.broadcasted_iota(jnp.int32, (mr, tile), 1)
    on_diag = rows_at == lanes_at
    mine = pivot[0]
    inv = 1.0 / jnp.sum(jnp.where(on_diag, mine, 0.0), axis=1, keepdims=True)
    mbuf[me] = jnp.where(on_diag, inv, mine * inv).astype(BF16)

    def masked(value, rank):
        level = lax.broadcasted_iota(jnp.int32, value.shape, 0)
        return jnp.where(level < rank, value.astype(F32), 0.0).astype(BF16)

    fbuf[me] = jnp.concatenate(
        [
            col_ut[0, 0],
            masked(col_vt[0, 0], col_rank[0, 0]),
            masked(row_ut[0, 0], row_rank[0, 0]),
            row_vt[0, 0],
        ],
        axis=1,
    )
    for k in range(2):
        cbuf[k][r] = masked(cbuf[k][r], cb_rank[0, 0, 0])

    greeted = 2 + len(peers) + has_left.astype(jnp.int32) + has_right.astype(jnp.int32)
    pl.semaphore_wait(barrier, greeted)

    def copy(ref, send, recv, target):
        return pltpu.make_async_remote_copy(
            src_ref=ref, dst_ref=ref, send_sem=send, recv_sem=recv, device_id=target, device_id_type=MESH
        )

    left_dev, right_dev = (front, r - 1, c), (front, r + 1, c)
    partner_dev = (front, r, partner)
    panel = (fbuf, mbuf)

    def pcopy(t, q, cc, k, target):
        slot = q * n_col + cc
        return copy(panel[t].at[slot], ssem_p.at[t, slot, k], rsem_p.at[t, slot], target)

    def zcopy(t, q, k, target):
        if t < 2:
            return pcopy(t, q, c, k, target)
        return copy(cbuf[t - 2].at[q], ssem_c.at[t - 2, q, k], rsem_c.at[t - 2, q], target)

    def z_start(t, q, to_right, to_left):
        if to_right:

            @pl.when(has_right)
            def _():
                zcopy(t, q, 2, right_dev).start()

        if to_left:

            @pl.when(has_left)
            def _():
                zcopy(t, q, 1, left_dev).start()

        if t < 2:
            for k, p in enumerate(peers):
                pcopy(t, q, c, 3 + k, (front, r, p)).start()
            pcopy(t, q, c, 0, partner_dev).start()

    def z_own(t):
        z_start(t, r, True, True)

    def z_rest(t):
        for s in range(1, n_row):

            @pl.when(r - s >= 0)
            def _():
                zcopy(t, r - s, 0, partner_dev).wait_recv()
                z_start(t, r - s, True, False)

            @pl.when(r + s < n_row)
            def _():
                zcopy(t, r + s, 0, partner_dev).wait_recv()
                z_start(t, r + s, False, True)

    others = [lax.rem(x + k, n_x) * 2 + 1 - core for k in range(n_x)]

    def panel_relay(t):
        for s in range(n_row):

            def relay(q):
                for p in peers:
                    pcopy(t, q, p, 0, partner_dev).wait_recv()
                    pcopy(t, q, p, 0, partner_dev).start()

            @pl.when(r - s >= 0)
            def _():
                relay(r - s)

            if s > 0:

                @pl.when(r + s < n_row)
                def _():
                    relay(r + s)

    def find(wanted):
        at, found = jnp.int32(0), jnp.int32(0)
        for i in range(pmap.shape[1]):
            hit = pmap[0, i] == wanted
            at, found = jnp.where(hit, i, at), jnp.where(hit, 1, found)
        return at, found.astype(F32)

    i_at = [find(2 * r + u) for u in range(2)]
    j_own, j_sib = find(2 * c + half), find(2 * c + 1 - half)

    def kept(value, flag):
        return (value.astype(F32) * flag).astype(BF16)

    def scopy(k, cc, lane, target):
        return copy(sbuf[k].at[cc], ssem_s.at[k, cc, lane], rsem_s.at[k, cc], target)

    def share(k):
        for u in range(2):
            at, found = i_at[u]
            value = cbuf[k][at]
            sbuf[k][c, u] = kept(value, found) if k < 2 else value
        for lane, p in enumerate(peers):
            scopy(k, c, 1 + lane, (front, r, p)).start()
        scopy(k, c, 0, partner_dev).start()

    def share_relay(k):
        for p in peers:
            scopy(k, p, 0, partner_dev).wait_recv()
            scopy(k, p, 0, partner_dev).start()

    ends = [(ybuf.at[k], zbuf.at[k]) for k in range(4)] + [(yr, zr), (yd, zd)]

    def ycopy(t):
        return pltpu.make_async_remote_copy(
            src_ref=ends[t][0],
            dst_ref=ends[t][1],
            send_sem=ssem_y.at[t],
            recv_sem=rsem_y.at[t],
            device_id=(sibling, r, c),
            device_id_type=MESH,
        )

    def across(k):
        for p in others:
            scopy(k, p, 0, partner_dev).wait_recv()
        for u in range(2):
            value = sbuf[k][j_sib[0], u]
            ybuf[k, u] = kept(value, j_sib[1]) if k < 2 else value
        ycopy(k).start()

    for t in range(3):
        z_own(t)
    z_rest(0)
    z_own(3)
    z_rest(1)
    z_own(4)
    z_rest(2)
    z_own(5)
    share(0)
    panel_relay(0)
    panel_relay(1)
    z_rest(3)
    share(1)
    for t in range(2):
        for q in range(n_row):
            for p in others:
                pcopy(t, q, p, 0, partner_dev).wait_recv()

    pivots = mbuf[...].reshape(tile, tile)
    diag_blocks = []
    lane_block = 128
    for b in range(tile // lane_block):
        total = jnp.zeros((1, lane_block), F32)
        for d in range(lane_block // mr):
            dev = b * (lane_block // mr) + d
            piece = mbuf[dev, :, b * lane_block : (b + 1) * lane_block].astype(F32)
            at_r = lax.broadcasted_iota(jnp.int32, piece.shape, 0) + d * mr
            at_l = lax.broadcasted_iota(jnp.int32, piece.shape, 1)
            total = total + jnp.sum(jnp.where(at_r == at_l, piece, 0.0), axis=0, keepdims=True)
        diag_blocks.append(total)
    diag = jnp.concatenate(diag_blocks, axis=1)

    def col_piece(at, first):
        return jnp.concatenate(
            [fbuf[at * n_col + k][:, first : first + wc] for k in range(n_col)], axis=1
        )

    def row_piece(at, first):
        return jnp.concatenate(
            [fbuf[k * n_col + at][:, first : first + wr] for k in range(n_row)], axis=1
        )

    v = jnp.concatenate([col_piece(i_at[u][0], wc) for u in range(2)], axis=0)
    v32 = v.astype(F32)
    t = v
    for step in range(3):
        t32 = v32 - (mm(t, pivots, ((1,), (0,))) - t.astype(F32) * diag)
        t = t32.astype(BF16)
    lower = (t32 * diag).astype(BF16)
    col_u = [col_piece(i_at[u][0], 0) for u in range(2)]

    def updates(j):
        at, found = j
        core_ = mm(lower, row_piece(at, 2 * wc), ((1,), (1,))).astype(BF16)
        return [
            (
                mm(core_[u * rank_dim : (u + 1) * rank_dim], col_u[u], ((0,), (0,)))
                * (-found * i_at[u][1])
            ).astype(BF16)
            for u in range(2)
        ]

    yr[...] = row_piece(j_sib[0], 2 * wc + wr)
    ycopy(4).start()
    for u, value in enumerate(updates(j_sib)):
        yd[u] = value
    ycopy(5).start()

    share_relay(0)
    z_rest(4)
    share(2)
    share_relay(1)
    across(0)
    z_rest(5)
    share(3)
    share_relay(2)
    across(1)
    own = updates(j_own)
    own_r = row_piece(j_own[0], 2 * wc + wr)
    share_relay(3)
    across(2)
    across(3)

    ycopy(4).wait_recv()
    ycopy(5).wait_recv()
    for k in range(2):
        ycopy(k).wait_recv()
    lefts = []
    for u in range(2):
        from_cb = [
            jnp.concatenate([kept(sbuf[k][j_own[0], u], j_own[1]) for k in range(2)], axis=1),
            jnp.concatenate([zbuf[k, u] for k in range(2)], axis=1),
        ]
        lefts.append(jnp.concatenate([from_cb[0], own[u], from_cb[1], zd[u]], axis=0))
    for k in range(2):
        ycopy(2 + k).wait_recv()
        lanes = slice(k * wide, (k + 1) * wide)
        for u in range(2):
            right = jnp.concatenate(
                [sbuf[2 + k][j_own[0], u], own_r[:, lanes], zbuf[2 + k, u], zr[:, lanes]], axis=0
            )
            out[0, u, 0, :, lanes] = mm(lefts[u], right, ((0,), (0,))).astype(BF16)

    for t in range(6):
        ycopy(t).wait_send()
    for k in range(4):
        for lane, p in enumerate(peers):
            scopy(k, c, 1 + lane, partner_dev).wait_send()
            scopy(k, p, 0, partner_dev).wait_send()
        scopy(k, c, 0, partner_dev).wait_send()
    for q in range(n_row):
        for t in range(2):
            for k, p in enumerate(peers):
                pcopy(t, q, c, 3 + k, partner_dev).wait_send()
                pcopy(t, q, p, 0, partner_dev).wait_send()
            pcopy(t, q, c, 0, partner_dev).wait_send()

        @pl.when((q <= r) & has_right)
        def _():
            for t in range(6):
                zcopy(t, q, 2, partner_dev).wait_send()

        @pl.when((q >= r) & has_left)
        def _():
            for t in range(6):
                zcopy(t, q, 1, partner_dev).wait_send()


def shards(
    n_row,
    n_col,
    pivot,
    col_ut,
    col_vt,
    col_rank,
    row_ut,
    row_vt,
    row_rank,
    cb_ut,
    cb_vt,
    cb_rank,
    parent_map,
):
    n_x = n_col // 2
    mr = pivot.shape[1]
    rank_dim, tile = cb_ut.shape[-2], cb_ut.shape[-1]
    width = 2 * col_ut.shape[-1] + 2 * row_ut.shape[-1]
    vmem = pl.BlockSpec(memory_space=pltpu.VMEM)
    hbm = pl.BlockSpec(memory_space=pltpu.HBM)
    pair = (2, rank_dim, tile)
    half = (rank_dim, tile // 2)
    dma = pltpu.SemaphoreType.DMA
    return pl.pallas_call(
        functools.partial(kernel, n_row, n_col),
        out_shape=jax.ShapeDtypeStruct((1, 2, 1, tile, tile), BF16),
        in_specs=[hbm] * 11,
        out_specs=vmem,
        scratch_shapes=[
            pltpu.VMEM(pivot.shape, F32),
            pltpu.VMEM(col_ut.shape, BF16),
            pltpu.VMEM(col_vt.shape, BF16),
            pltpu.VMEM(row_ut.shape, BF16),
            pltpu.VMEM(row_vt.shape, BF16),
            pltpu.SMEM(col_rank.shape, jnp.int32),
            pltpu.SMEM(row_rank.shape, jnp.int32),
            pltpu.SMEM(cb_rank.shape, jnp.int32),
            pltpu.SMEM(parent_map.shape, jnp.int32),
            pltpu.VMEM((n_row * n_col, mr, tile), BF16),
            pltpu.VMEM((n_row * n_col, rank_dim, width), BF16),
            *[pltpu.VMEM((n_row,) + half, BF16)] * 4,
            *[pltpu.VMEM((n_col, 2) + half, BF16)] * 4,
            pltpu.VMEM((4, 2) + half, BF16),
            pltpu.VMEM(pair, BF16),
            pltpu.VMEM(pair[1:], BF16),
            pltpu.VMEM((4, 2) + half, BF16),
            pltpu.VMEM(pair, BF16),
            pltpu.VMEM(pair[1:], BF16),
            dma((13,)),
            dma((2, n_row * n_col)),
            dma((2, n_row * n_col, 2 + n_x)),
            dma((4, n_row)),
            dma((4, n_row, 3)),
            dma((4, n_col)),
            dma((4, n_col, n_x)),
            dma((6,)),
            dma((6,)),
        ],
        compiler_params=pltpu.CompilerParams(
            collective_id=0, has_side_effects=True, vmem_limit_bytes=67043328
        ),
    )(
        pivot,
        col_ut,
        col_vt,
        row_ut,
        row_vt,
        cb_ut,
        cb_vt,
        col_rank,
        row_rank,
        cb_rank,
        parent_map,
    )


def solution(mesh):
    placed = (
        P("front", ("row", "col"), None),
        P("front", "row", None, "col"),
        P("front", "row", None, "col"),
        P("front", "row"),
        P("front", "col", None, "row"),
        P("front", "col", None, "row"),
        P("front", "col"),
        P("front", "row", "col", None, None),
        P("front", "row", "col", None, None),
        P("front", "row", "col"),
        P("front", None),
    )
    return jax.shard_map(
        functools.partial(shards, mesh.shape["row"], mesh.shape["col"]),
        mesh=mesh,
        in_specs=placed,
        out_specs=P("front", "row", "col", None, None),
        check_vma=False,
    )
```

```python
import functools

import jax
import jax.numpy as jnp
from jax import lax
from jax.experimental import pallas as pl
from jax.experimental.pallas import tpu as pltpu
from jax.sharding import PartitionSpec as P

MESH = pl.DeviceIdType.MESH
F32 = jnp.float32
BF16 = jnp.bfloat16


def mm(a, b, dims):
    return lax.dot_general(a, b, (dims, ((), ())), preferred_element_type=F32)


def kernel(
    n_row,
    n_col,
    pivot_hbm,
    col_ut_hbm,
    col_vt_hbm,
    row_ut_hbm,
    row_vt_hbm,
    cb_ut_hbm,
    cb_vt_hbm,
    col_rank_hbm,
    row_rank_hbm,
    cb_rank_hbm,
    pmap_hbm,
    out,
    pivot,
    col_ut,
    col_vt,
    row_ut,
    row_vt,
    col_rank,
    row_rank,
    cb_rank,
    pmap,
    mbuf,
    fbuf,
    c0,
    c1,
    c2,
    c3,
    s0,
    s1,
    s2,
    s3,
    ybuf,
    yd,
    yr,
    zbuf,
    zd,
    zr,
    in_sem,
    rsem_p,
    ssem_p,
    rsem_c,
    ssem_c,
    rsem_s,
    ssem_s,
    rsem_y,
    ssem_y,
):
    cbuf, sbuf = (c0, c1, c2, c3), (s0, s1, s2, s3)
    front, r, c = lax.axis_index("front"), lax.axis_index("row"), lax.axis_index("col")
    n_x = n_col // 2
    x, core = c // 2, c % 2
    partner = 2 * x + 1 - core
    sibling = front + 1 - 2 * (front % 2)
    half = front % 2
    peers = [lax.rem(x + k, n_x) * 2 + core for k in range(1, n_x)]
    wc, wr = col_ut.shape[-1], row_ut.shape[-1]
    rank_dim, tile = cb_ut_hbm.shape[-2], cb_ut_hbm.shape[-1]
    wide = tile // 2
    mr = pivot.shape[1]
    has_left, has_right = r > 0, r < n_row - 1

    def chunk_src(k):
        return (cb_ut_hbm, cb_vt_hbm)[k // 2].at[0, 0, 0, :, pl.ds(k % 2 * wide, wide)]

    loads = [
        pltpu.make_async_copy(src, dst, in_sem.at[k])
        for k, (src, dst) in enumerate(
            [
                (pivot_hbm, pivot),
                (col_rank_hbm, col_rank),
                (row_rank_hbm, row_rank),
                (cb_rank_hbm, cb_rank),
                (pmap_hbm, pmap),
                (col_ut_hbm, col_ut),
                (col_vt_hbm, col_vt),
                (row_ut_hbm, row_ut),
                (row_vt_hbm, row_vt),
            ]
            + [(chunk_src(k), cbuf[k].at[r]) for k in range(4)]
        )
    ]
    for load in loads:
        load.start()

    barrier = pltpu.get_barrier_semaphore()

    def greet(target):
        pl.semaphore_signal(barrier, inc=1, device_id=target, device_id_type=MESH)

    greet((sibling, r, c))
    greet((front, r, partner))
    for p in peers:
        greet((front, r, p))

    @pl.when(has_left)
    def _():
        greet((front, r - 1, c))

    @pl.when(has_right)
    def _():
        greet((front, r + 1, c))

    for load in loads:
        load.wait()
    me = r * n_col + c
    rows_at = lax.broadcasted_iota(jnp.int32, (mr, tile), 0) + me * mr
    lanes_at = lax.broadcasted_iota(jnp.int32, (mr, tile), 1)
    on_diag = rows_at == lanes_at
    mine = pivot[0]
    inv = 1.0 / jnp.sum(jnp.where(on_diag, mine, 0.0), axis=1, keepdims=True)
    mbuf[me] = jnp.where(on_diag, inv, mine * inv).astype(BF16)

    def masked(value, rank):
        level = lax.broadcasted_iota(jnp.int32, value.shape, 0)
        return jnp.where(level < rank, value.astype(F32), 0.0).astype(BF16)

    fbuf[me] = jnp.concatenate(
        [
            col_ut[0, 0],
            masked(col_vt[0, 0], col_rank[0, 0]),
            masked(row_ut[0, 0], row_rank[0, 0]),
            row_vt[0, 0],
        ],
        axis=1,
    )
    for k in range(2):
        cbuf[k][r] = masked(cbuf[k][r], cb_rank[0, 0, 0])

    greeted = 2 + len(peers) + has_left.astype(jnp.int32) + has_right.astype(jnp.int32)
    pl.semaphore_wait(barrier, greeted)

    def copy(ref, send, recv, target):
        return pltpu.make_async_remote_copy(
            src_ref=ref, dst_ref=ref, send_sem=send, recv_sem=recv, device_id=target, device_id_type=MESH
        )

    left_dev, right_dev = (front, r - 1, c), (front, r + 1, c)
    partner_dev = (front, r, partner)
    panel = (fbuf, mbuf)

    def pcopy(t, q, cc, k, target):
        slot = q * n_col + cc
        return copy(panel[t].at[slot], ssem_p.at[t, slot, k], rsem_p.at[t, slot], target)

    def zcopy(t, q, k, target):
        if t < 2:
            return pcopy(t, q, c, k, target)
        return copy(cbuf[t - 2].at[q], ssem_c.at[t - 2, q, k], rsem_c.at[t - 2, q], target)

    def z_start(t, q, to_right, to_left):
        if to_right:

            @pl.when(has_right)
            def _():
                zcopy(t, q, 2, right_dev).start()

        if to_left:

            @pl.when(has_left)
            def _():
                zcopy(t, q, 1, left_dev).start()

        if t < 2:
            for k, p in enumerate(peers):
                pcopy(t, q, c, 3 + k, (front, r, p)).start()
            pcopy(t, q, c, 0, partner_dev).start()

    def z_own(t):
        z_start(t, r, True, True)

    def z_hop(t, s):
        @pl.when(r - s >= 0)
        def _():
            zcopy(t, r - s, 0, partner_dev).wait_recv()
            z_start(t, r - s, True, False)

        @pl.when(r + s < n_row)
        def _():
            zcopy(t, r + s, 0, partner_dev).wait_recv()
            z_start(t, r + s, False, True)

    others = [lax.rem(x + k, n_x) * 2 + 1 - core for k in range(n_x)]

    def panel_relay(t, s):
        def relay(q):
            for p in peers:
                pcopy(t, q, p, 0, partner_dev).wait_recv()
                pcopy(t, q, p, 0, partner_dev).start()

        @pl.when(r - s >= 0)
        def _():
            relay(r - s)

        if s > 0:

            @pl.when(r + s < n_row)
            def _():
                relay(r + s)

    def find(wanted):
        at, found = jnp.int32(0), jnp.int32(0)
        for i in range(pmap.shape[1]):
            hit = pmap[0, i] == wanted
            at, found = jnp.where(hit, i, at), jnp.where(hit, 1, found)
        return at, found.astype(F32)

    i_at = [find(2 * r + u) for u in range(2)]
    j_own, j_sib = find(2 * c + half), find(2 * c + 1 - half)

    def kept(value, flag):
        return (value.astype(F32) * flag).astype(BF16)

    def scopy(k, cc, lane, target):
        return copy(sbuf[k].at[cc], ssem_s.at[k, cc, lane], rsem_s.at[k, cc], target)

    def share(k):
        for u in range(2):
            at, found = i_at[u]
            value = cbuf[k][at]
            sbuf[k][c, u] = kept(value, found) if k < 2 else value
        for lane, p in enumerate(peers):
            scopy(k, c, 1 + lane, (front, r, p)).start()
        scopy(k, c, 0, partner_dev).start()

    def share_relay(k):
        for p in peers:
            scopy(k, p, 0, partner_dev).wait_recv()
            scopy(k, p, 0, partner_dev).start()

    ends = [(ybuf.at[k], zbuf.at[k]) for k in range(4)] + [(yr, zr), (yd, zd)]

    def ycopy(t):
        return pltpu.make_async_remote_copy(
            src_ref=ends[t][0],
            dst_ref=ends[t][1],
            send_sem=ssem_y.at[t],
            recv_sem=rsem_y.at[t],
            device_id=(sibling, r, c),
            device_id_type=MESH,
        )

    def across(k):
        for p in others:
            scopy(k, p, 0, partner_dev).wait_recv()
        for u in range(2):
            value = sbuf[k][j_sib[0], u]
            ybuf[k, u] = kept(value, j_sib[1]) if k < 2 else value
        ycopy(k).start()

    def col_piece(at, first):
        return jnp.concatenate(
            [fbuf[at * n_col + k][:, first : first + wc] for k in range(n_col)], axis=1
        )

    def row_piece(at, first):
        return jnp.concatenate(
            [fbuf[k * n_col + at][:, first : first + wr] for k in range(n_row)], axis=1
        )

    def updates(lower, col_u, j):
        at, found = j
        core_ = mm(lower, row_piece(at, 2 * wc), ((1,), (1,))).astype(BF16)
        return [
            (
                mm(core_[u * rank_dim : (u + 1) * rank_dim], col_u[u], ((0,), (0,)))
                * (-found * i_at[u][1])
            ).astype(BF16)
            for u in range(2)
        ]

    def pivoting():
        for t in range(2):
            for q in range(n_row):
                for p in others:
                    pcopy(t, q, p, 0, partner_dev).wait_recv()
        yr[...] = row_piece(j_sib[0], 2 * wc + wr)
        ycopy(4).start()
        pivots = mbuf[...].reshape(tile, tile)
        diag_blocks = []
        lane_block = 128
        for b in range(tile // lane_block):
            total = jnp.zeros((1, lane_block), F32)
            for d in range(lane_block // mr):
                dev = b * (lane_block // mr) + d
                piece = mbuf[dev, :, b * lane_block : (b + 1) * lane_block].astype(F32)
                at_r = lax.broadcasted_iota(jnp.int32, piece.shape, 0) + d * mr
                at_l = lax.broadcasted_iota(jnp.int32, piece.shape, 1)
                total = total + jnp.sum(jnp.where(at_r == at_l, piece, 0.0), axis=0, keepdims=True)
            diag_blocks.append(total)
        diag = jnp.concatenate(diag_blocks, axis=1)
        v = jnp.concatenate([col_piece(i_at[u][0], wc) for u in range(2)], axis=0)
        v32 = v.astype(F32)
        t = v
        for step in range(3):
            t32 = v32 - (mm(t, pivots, ((1,), (0,))) - t.astype(F32) * diag)
            t = t32.astype(BF16)
        lower = (t32 * diag).astype(BF16)
        col_u = [col_piece(i_at[u][0], 0) for u in range(2)]
        for u, value in enumerate(updates(lower, col_u, j_sib)):
            yd[u] = value
        ycopy(5).start()
        return updates(lower, col_u, j_own), row_piece(j_own[0], 2 * wc + wr)

    last, ahead = n_row - 1, 3
    for t in range(ahead + 1):
        z_own(t)
    for d in range(1, last + 9):
        if ahead + d < 6:
            z_own(ahead + d)
        for s in range(last, 0, -1):
            if 0 <= d - s < 6:
                z_hop(d - s, s)
        if 0 <= d - last - 2 < 4:
            share(d - last - 2)
        for t in range(2):
            if 0 <= d - t - 1 <= last:
                panel_relay(t, d - t - 1)
        if d == last + 3:
            own, own_r = pivoting()
        if 0 <= d - last - 4 < 4:
            share_relay(d - last - 4)
        if 0 <= d - last - 5 < 4:
            across(d - last - 5)

    ycopy(4).wait_recv()
    ycopy(5).wait_recv()
    for k in range(2):
        ycopy(k).wait_recv()
    lefts = []
    for u in range(2):
        from_cb = [
            jnp.concatenate([kept(sbuf[k][j_own[0], u], j_own[1]) for k in range(2)], axis=1),
            jnp.concatenate([zbuf[k, u] for k in range(2)], axis=1),
        ]
        lefts.append(jnp.concatenate([from_cb[0], own[u], from_cb[1], zd[u]], axis=0))
    for k in range(2):
        ycopy(2 + k).wait_recv()
        lanes = slice(k * wide, (k + 1) * wide)
        for u in range(2):
            right = jnp.concatenate(
                [sbuf[2 + k][j_own[0], u], own_r[:, lanes], zbuf[2 + k, u], zr[:, lanes]], axis=0
            )
            out[0, u, 0, :, lanes] = mm(lefts[u], right, ((0,), (0,))).astype(BF16)

    for t in range(6):
        ycopy(t).wait_send()
    for k in range(4):
        for lane, p in enumerate(peers):
            scopy(k, c, 1 + lane, partner_dev).wait_send()
            scopy(k, p, 0, partner_dev).wait_send()
        scopy(k, c, 0, partner_dev).wait_send()
    for q in range(n_row):
        for t in range(2):
            for k, p in enumerate(peers):
                pcopy(t, q, c, 3 + k, partner_dev).wait_send()
                pcopy(t, q, p, 0, partner_dev).wait_send()
            pcopy(t, q, c, 0, partner_dev).wait_send()

        @pl.when((q <= r) & has_right)
        def _():
            for t in range(6):
                zcopy(t, q, 2, partner_dev).wait_send()

        @pl.when((q >= r) & has_left)
        def _():
            for t in range(6):
                zcopy(t, q, 1, partner_dev).wait_send()


def shards(
    n_row,
    n_col,
    pivot,
    col_ut,
    col_vt,
    col_rank,
    row_ut,
    row_vt,
    row_rank,
    cb_ut,
    cb_vt,
    cb_rank,
    parent_map,
):
    n_x = n_col // 2
    mr = pivot.shape[1]
    rank_dim, tile = cb_ut.shape[-2], cb_ut.shape[-1]
    width = 2 * col_ut.shape[-1] + 2 * row_ut.shape[-1]
    vmem = pl.BlockSpec(memory_space=pltpu.VMEM)
    hbm = pl.BlockSpec(memory_space=pltpu.HBM)
    pair = (2, rank_dim, tile)
    half = (rank_dim, tile // 2)
    dma = pltpu.SemaphoreType.DMA
    return pl.pallas_call(
        functools.partial(kernel, n_row, n_col),
        out_shape=jax.ShapeDtypeStruct((1, 2, 1, tile, tile), BF16),
        in_specs=[hbm] * 11,
        out_specs=vmem,
        scratch_shapes=[
            pltpu.VMEM(pivot.shape, F32),
            pltpu.VMEM(col_ut.shape, BF16),
            pltpu.VMEM(col_vt.shape, BF16),
            pltpu.VMEM(row_ut.shape, BF16),
            pltpu.VMEM(row_vt.shape, BF16),
            pltpu.SMEM(col_rank.shape, jnp.int32),
            pltpu.SMEM(row_rank.shape, jnp.int32),
            pltpu.SMEM(cb_rank.shape, jnp.int32),
            pltpu.SMEM(parent_map.shape, jnp.int32),
            pltpu.VMEM((n_row * n_col, mr, tile), BF16),
            pltpu.VMEM((n_row * n_col, rank_dim, width), BF16),
            *[pltpu.VMEM((n_row,) + half, BF16)] * 4,
            *[pltpu.VMEM((n_col, 2) + half, BF16)] * 4,
            pltpu.VMEM((4, 2) + half, BF16),
            pltpu.VMEM(pair, BF16),
            pltpu.VMEM(pair[1:], BF16),
            pltpu.VMEM((4, 2) + half, BF16),
            pltpu.VMEM(pair, BF16),
            pltpu.VMEM(pair[1:], BF16),
            dma((13,)),
            dma((2, n_row * n_col)),
            dma((2, n_row * n_col, 2 + n_x)),
            dma((4, n_row)),
            dma((4, n_row, 3)),
            dma((4, n_col)),
            dma((4, n_col, n_x)),
            dma((6,)),
            dma((6,)),
        ],
        compiler_params=pltpu.CompilerParams(
            collective_id=0, has_side_effects=True, vmem_limit_bytes=67043328
        ),
    )(
        pivot,
        col_ut,
        col_vt,
        row_ut,
        row_vt,
        cb_ut,
        cb_vt,
        col_rank,
        row_rank,
        cb_rank,
        parent_map,
    )


def solution(mesh):
    placed = (
        P("front", ("row", "col"), None),
        P("front", "row", None, "col"),
        P("front", "row", None, "col"),
        P("front", "row"),
        P("front", "col", None, "row"),
        P("front", "col", None, "row"),
        P("front", "col"),
        P("front", "row", "col", None, None),
        P("front", "row", "col", None, None),
        P("front", "row", "col"),
        P("front", None),
    )
    return jax.shard_map(
        functools.partial(shards, mesh.shape["row"], mesh.shape["col"]),
        mesh=mesh,
        in_specs=placed,
        out_specs=P("front", "row", "col", None, None),
        check_vma=False,
    )
```

```python
import functools

import jax
import jax.numpy as jnp
from jax import lax
from jax.experimental import pallas as pl
from jax.experimental.pallas import tpu as pltpu
from jax.sharding import PartitionSpec as P

MESH = pl.DeviceIdType.MESH
F32 = jnp.float32
BF16 = jnp.bfloat16


def mm(a, b, dims):
    return lax.dot_general(a, b, (dims, ((), ())), preferred_element_type=F32)


def kernel(
    n_row,
    n_col,
    pivot_hbm,
    col_ut_hbm,
    col_vt_hbm,
    row_ut_hbm,
    row_vt_hbm,
    cb_ut_hbm,
    cb_vt_hbm,
    col_rank_hbm,
    row_rank_hbm,
    cb_rank_hbm,
    pmap_hbm,
    out,
    pivot,
    col_ut,
    col_vt,
    row_ut,
    row_vt,
    col_rank,
    row_rank,
    cb_rank,
    pmap,
    mbuf,
    fbuf,
    c0,
    c1,
    c2,
    c3,
    s0,
    s1,
    s2,
    s3,
    ybuf,
    yd,
    yr,
    zbuf,
    zd,
    zr,
    in_sem,
    rsem_p,
    ssem_p,
    rsem_c,
    ssem_c,
    rsem_s,
    ssem_s,
    rsem_y,
    ssem_y,
):
    cbuf, sbuf = (c0, c1, c2, c3), (s0, s1, s2, s3)
    front, r, c = lax.axis_index("front"), lax.axis_index("row"), lax.axis_index("col")
    n_x = n_col // 2
    x, core = c // 2, c % 2
    partner = 2 * x + 1 - core
    sibling = front + 1 - 2 * (front % 2)
    half = front % 2
    peers = [lax.rem(x + k, n_x) * 2 + core for k in range(1, n_x)]
    wc, wr = col_ut.shape[-1], row_ut.shape[-1]
    rank_dim, tile = cb_ut_hbm.shape[-2], cb_ut_hbm.shape[-1]
    wide = tile // 2
    mr = pivot.shape[1]
    has_left, has_right = r > 0, r < n_row - 1

    def chunk_src(k):
        return (cb_ut_hbm, cb_vt_hbm)[k // 2].at[0, 0, 0, :, pl.ds(k % 2 * wide, wide)]

    loads = [
        pltpu.make_async_copy(src, dst, in_sem.at[k])
        for k, (src, dst) in enumerate(
            [
                (pivot_hbm, pivot),
                (col_rank_hbm, col_rank),
                (row_rank_hbm, row_rank),
                (cb_rank_hbm, cb_rank),
                (pmap_hbm, pmap),
                (col_ut_hbm, col_ut),
                (col_vt_hbm, col_vt),
                (row_ut_hbm, row_ut),
                (row_vt_hbm, row_vt),
            ]
            + [(chunk_src(k), cbuf[k].at[r]) for k in range(4)]
        )
    ]
    for load in loads:
        load.start()

    barrier = pltpu.get_barrier_semaphore()

    def greet(target):
        pl.semaphore_signal(barrier, inc=1, device_id=target, device_id_type=MESH)

    greet((sibling, r, c))
    greet((front, r, partner))
    for p in peers:
        greet((front, r, p))

    @pl.when(has_left)
    def _():
        greet((front, r - 1, c))

    @pl.when(has_right)
    def _():
        greet((front, r + 1, c))

    for load in loads:
        load.wait()
    me = r * n_col + c
    rows_at = lax.broadcasted_iota(jnp.int32, (mr, tile), 0) + me * mr
    lanes_at = lax.broadcasted_iota(jnp.int32, (mr, tile), 1)
    on_diag = rows_at == lanes_at
    mine = pivot[0]
    inv = 1.0 / jnp.sum(jnp.where(on_diag, mine, 0.0), axis=1, keepdims=True)
    mbuf[me] = jnp.where(on_diag, inv, mine * inv).astype(BF16)

    def masked(value, rank):
        level = lax.broadcasted_iota(jnp.int32, value.shape, 0)
        return jnp.where(level < rank, value.astype(F32), 0.0).astype(BF16)

    fbuf[me] = jnp.concatenate(
        [
            col_ut[0, 0],
            masked(col_vt[0, 0], col_rank[0, 0]),
            masked(row_ut[0, 0], row_rank[0, 0]),
            row_vt[0, 0],
        ],
        axis=1,
    )
    for k in range(2):
        cbuf[k][r] = masked(cbuf[k][r], cb_rank[0, 0, 0])

    greeted = 2 + len(peers) + has_left.astype(jnp.int32) + has_right.astype(jnp.int32)
    pl.semaphore_wait(barrier, greeted)

    def copy(ref, send, recv, target):
        return pltpu.make_async_remote_copy(
            src_ref=ref, dst_ref=ref, send_sem=send, recv_sem=recv, device_id=target, device_id_type=MESH
        )

    left_dev, right_dev = (front, r - 1, c), (front, r + 1, c)
    partner_dev = (front, r, partner)
    panel = (fbuf, mbuf)

    def pcopy(t, q, cc, k, target):
        slot = q * n_col + cc
        return copy(panel[t].at[slot], ssem_p.at[t, slot, k], rsem_p.at[t, slot], target)

    def zcopy(t, q, k, target):
        if t < 2:
            return pcopy(t, q, c, k, target)
        return copy(cbuf[t - 2].at[q], ssem_c.at[t - 2, q, k], rsem_c.at[t - 2, q], target)

    def z_start(t, q, to_right, to_left):
        if to_right:

            @pl.when(has_right)
            def _():
                zcopy(t, q, 2, right_dev).start()

        if to_left:

            @pl.when(has_left)
            def _():
                zcopy(t, q, 1, left_dev).start()

        if t < 2:
            for k, p in enumerate(peers):
                pcopy(t, q, c, 3 + k, (front, r, p)).start()
            pcopy(t, q, c, 0, partner_dev).start()

    def z_own(t):
        z_start(t, r, True, True)

    def z_hop(t, s):
        @pl.when(r - s >= 0)
        def _():
            zcopy(t, r - s, 0, partner_dev).wait_recv()
            z_start(t, r - s, True, False)

        @pl.when(r + s < n_row)
        def _():
            zcopy(t, r + s, 0, partner_dev).wait_recv()
            z_start(t, r + s, False, True)

    others = [lax.rem(x + k, n_x) * 2 + 1 - core for k in range(n_x)]

    def panel_relay(t, s):
        def relay(q):
            for p in peers:
                pcopy(t, q, p, 0, partner_dev).wait_recv()
                pcopy(t, q, p, 0, partner_dev).start()

        @pl.when(r - s >= 0)
        def _():
            relay(r - s)

        if s > 0:

            @pl.when(r + s < n_row)
            def _():
                relay(r + s)

    def find(wanted):
        at, found = jnp.int32(0), jnp.int32(0)
        for i in range(pmap.shape[1]):
            hit = pmap[0, i] == wanted
            at, found = jnp.where(hit, i, at), jnp.where(hit, 1, found)
        return at, found.astype(F32)

    i_at = [find(2 * r + u) for u in range(2)]
    j_own, j_sib = find(2 * c + half), find(2 * c + 1 - half)

    def kept(value, flag):
        return (value.astype(F32) * flag).astype(BF16)

    def scopy(k, cc, lane, target):
        return copy(sbuf[k].at[cc], ssem_s.at[k, cc, lane], rsem_s.at[k, cc], target)

    def share(k):
        for u in range(2):
            at, found = i_at[u]
            value = cbuf[k][at]
            sbuf[k][c, u] = kept(value, found) if k < 2 else value
        for lane, p in enumerate(peers):
            scopy(k, c, 1 + lane, (front, r, p)).start()
        scopy(k, c, 0, partner_dev).start()

    def share_relay(k):
        for p in peers:
            scopy(k, p, 0, partner_dev).wait_recv()
            scopy(k, p, 0, partner_dev).start()

    ends = [(ybuf.at[k], zbuf.at[k]) for k in range(4)] + [(yr, zr), (yd, zd)]

    def ycopy(t):
        return pltpu.make_async_remote_copy(
            src_ref=ends[t][0],
            dst_ref=ends[t][1],
            send_sem=ssem_y.at[t],
            recv_sem=rsem_y.at[t],
            device_id=(sibling, r, c),
            device_id_type=MESH,
        )

    def across(k):
        for p in others:
            scopy(k, p, 0, partner_dev).wait_recv()
        for u in range(2):
            value = sbuf[k][j_sib[0], u]
            ybuf[k, u] = kept(value, j_sib[1]) if k < 2 else value
        ycopy(k).start()

    def col_piece(at, first):
        return jnp.concatenate(
            [fbuf[at * n_col + k][:, first : first + wc] for k in range(n_col)], axis=1
        )

    def row_piece(at, first):
        return jnp.concatenate(
            [fbuf[k * n_col + at][:, first : first + wr] for k in range(n_row)], axis=1
        )

    def updates(lower, col_u, j):
        at, found = j
        core_ = mm(lower, row_piece(at, 2 * wc), ((1,), (1,))).astype(BF16)
        return [
            (
                mm(core_[u * rank_dim : (u + 1) * rank_dim], col_u[u], ((0,), (0,)))
                * (-found * i_at[u][1])
            ).astype(BF16)
            for u in range(2)
        ]

    def pivoting():
        for t in range(2):
            for q in range(n_row):
                for p in others:
                    pcopy(t, q, p, 0, partner_dev).wait_recv()
        yr[...] = row_piece(j_sib[0], 2 * wc + wr)
        ycopy(4).start()
        pivots = mbuf[...].reshape(tile, tile)
        diag_blocks = []
        lane_block = 128
        for b in range(tile // lane_block):
            total = jnp.zeros((1, lane_block), F32)
            for d in range(lane_block // mr):
                dev = b * (lane_block // mr) + d
                piece = mbuf[dev, :, b * lane_block : (b + 1) * lane_block].astype(F32)
                at_r = lax.broadcasted_iota(jnp.int32, piece.shape, 0) + d * mr
                at_l = lax.broadcasted_iota(jnp.int32, piece.shape, 1)
                total = total + jnp.sum(jnp.where(at_r == at_l, piece, 0.0), axis=0, keepdims=True)
            diag_blocks.append(total)
        diag = jnp.concatenate(diag_blocks, axis=1)
        v = jnp.concatenate([col_piece(i_at[u][0], wc) for u in range(2)], axis=0)
        v32 = v.astype(F32)
        t = v
        for step in range(3):
            t32 = v32 - (mm(t, pivots, ((1,), (0,))) - t.astype(F32) * diag)
            t = t32.astype(BF16)
        lower = (t32 * diag).astype(BF16)
        col_u = [col_piece(i_at[u][0], 0) for u in range(2)]
        for u, value in enumerate(updates(lower, col_u, j_sib)):
            yd[u] = value
        ycopy(5).start()
        return updates(lower, col_u, j_own), row_piece(j_own[0], 2 * wc + wr)

    last, lag = n_row - 1, 3
    for t in range(6):
        z_own(t)
    for d in range(lag * last + 11):
        for s in range(last, 0, -1):
            if 0 <= d - lag * s < 6:
                z_hop(d - lag * s, s)
        k = d - lag * last - 2
        if 0 <= k < 4:
            share(k)
        for t in range(2):
            for s in range(n_row):
                if d - t - 2 == lag * s:
                    panel_relay(t, s)
        if k == 2:
            own, own_r = pivoting()
        if 0 <= k - 3 < 4:
            share_relay(k - 3)
        if 0 <= k - 5 < 4:
            across(k - 5)

    ycopy(4).wait_recv()
    ycopy(5).wait_recv()
    for k in range(2):
        ycopy(k).wait_recv()
    lefts = []
    for u in range(2):
        from_cb = [
            jnp.concatenate([kept(sbuf[k][j_own[0], u], j_own[1]) for k in range(2)], axis=1),
            jnp.concatenate([zbuf[k, u] for k in range(2)], axis=1),
        ]
        lefts.append(jnp.concatenate([from_cb[0], own[u], from_cb[1], zd[u]], axis=0))
    for k in range(2):
        ycopy(2 + k).wait_recv()
        lanes = slice(k * wide, (k + 1) * wide)
        for u in range(2):
            right = jnp.concatenate(
                [sbuf[2 + k][j_own[0], u], own_r[:, lanes], zbuf[2 + k, u], zr[:, lanes]], axis=0
            )
            out[0, u, 0, :, lanes] = mm(lefts[u], right, ((0,), (0,))).astype(BF16)

    for t in range(6):
        ycopy(t).wait_send()
    for k in range(4):
        for lane, p in enumerate(peers):
            scopy(k, c, 1 + lane, partner_dev).wait_send()
            scopy(k, p, 0, partner_dev).wait_send()
        scopy(k, c, 0, partner_dev).wait_send()
    for q in range(n_row):
        for t in range(2):
            for k, p in enumerate(peers):
                pcopy(t, q, c, 3 + k, partner_dev).wait_send()
                pcopy(t, q, p, 0, partner_dev).wait_send()
            pcopy(t, q, c, 0, partner_dev).wait_send()

        @pl.when((q <= r) & has_right)
        def _():
            for t in range(6):
                zcopy(t, q, 2, partner_dev).wait_send()

        @pl.when((q >= r) & has_left)
        def _():
            for t in range(6):
                zcopy(t, q, 1, partner_dev).wait_send()


def shards(
    n_row,
    n_col,
    pivot,
    col_ut,
    col_vt,
    col_rank,
    row_ut,
    row_vt,
    row_rank,
    cb_ut,
    cb_vt,
    cb_rank,
    parent_map,
):
    n_x = n_col // 2
    mr = pivot.shape[1]
    rank_dim, tile = cb_ut.shape[-2], cb_ut.shape[-1]
    width = 2 * col_ut.shape[-1] + 2 * row_ut.shape[-1]
    vmem = pl.BlockSpec(memory_space=pltpu.VMEM)
    hbm = pl.BlockSpec(memory_space=pltpu.HBM)
    pair = (2, rank_dim, tile)
    half = (rank_dim, tile // 2)
    dma = pltpu.SemaphoreType.DMA
    return pl.pallas_call(
        functools.partial(kernel, n_row, n_col),
        out_shape=jax.ShapeDtypeStruct((1, 2, 1, tile, tile), BF16),
        in_specs=[hbm] * 11,
        out_specs=vmem,
        scratch_shapes=[
            pltpu.VMEM(pivot.shape, F32),
            pltpu.VMEM(col_ut.shape, BF16),
            pltpu.VMEM(col_vt.shape, BF16),
            pltpu.VMEM(row_ut.shape, BF16),
            pltpu.VMEM(row_vt.shape, BF16),
            pltpu.SMEM(col_rank.shape, jnp.int32),
            pltpu.SMEM(row_rank.shape, jnp.int32),
            pltpu.SMEM(cb_rank.shape, jnp.int32),
            pltpu.SMEM(parent_map.shape, jnp.int32),
            pltpu.VMEM((n_row * n_col, mr, tile), BF16),
            pltpu.VMEM((n_row * n_col, rank_dim, width), BF16),
            *[pltpu.VMEM((n_row,) + half, BF16)] * 4,
            *[pltpu.VMEM((n_col, 2) + half, BF16)] * 4,
            pltpu.VMEM((4, 2) + half, BF16),
            pltpu.VMEM(pair, BF16),
            pltpu.VMEM(pair[1:], BF16),
            pltpu.VMEM((4, 2) + half, BF16),
            pltpu.VMEM(pair, BF16),
            pltpu.VMEM(pair[1:], BF16),
            dma((13,)),
            dma((2, n_row * n_col)),
            dma((2, n_row * n_col, 2 + n_x)),
            dma((4, n_row)),
            dma((4, n_row, 3)),
            dma((4, n_col)),
            dma((4, n_col, n_x)),
            dma((6,)),
            dma((6,)),
        ],
        compiler_params=pltpu.CompilerParams(
            collective_id=0, has_side_effects=True, vmem_limit_bytes=67043328
        ),
    )(
        pivot,
        col_ut,
        col_vt,
        row_ut,
        row_vt,
        cb_ut,
        cb_vt,
        col_rank,
        row_rank,
        cb_rank,
        parent_map,
    )


def solution(mesh):
    placed = (
        P("front", ("row", "col"), None),
        P("front", "row", None, "col"),
        P("front", "row", None, "col"),
        P("front", "row"),
        P("front", "col", None, "row"),
        P("front", "col", None, "row"),
        P("front", "col"),
        P("front", "row", "col", None, None),
        P("front", "row", "col", None, None),
        P("front", "row", "col"),
        P("front", None),
    )
    return jax.shard_map(
        functools.partial(shards, mesh.shape["row"], mesh.shape["col"]),
        mesh=mesh,
        in_specs=placed,
        out_specs=P("front", "row", "col", None, None),
        check_vma=False,
    )
```
